32 devices in a mesh: rows: 8 (over z, y), grp: 4 (over x, core).
Axes of the slice: x: 2, y: 2, z: 4, core: 2. Of those that a mesh axis runs over, the one named last changes fastest.
Arguments:
- modes: float32 [393216, 256], P(('rows', 'grp')), may hold values from -6 to 6
- points: int32 [196], replicated, may hold values from 0 to 393215, as said below
Outputs:
- residual: float32 [393216, 128], P(('rows', 'grp'))
- norms: float32 [4, 128], replicated
The draws below stay inside these ranges and needn't reach their ends.
Inputs may be any that keep to these rules, and one draw needn't show every extreme that they name: `points`: distinct row indices of the mode matrix.
All inputs are finite; a program needn't handle non-finite values.
Results may differ from the reference program's by a relative error of at most 0.00029.
Values sent between devices are 32-bit elements; how exact they have to be, the bound alone decides.
A program may use at most 128 MiB of HBM per device.

```python
import jax
import jax.numpy as jnp
from jax import lax

MODES = 256
FIT = 128
ROWS_DEV = 12288
PRIOR = 192
STEPS = 4
NPTS = 196
ROWS = 393216
N_ROWS = 8
N_GRP = 4


def draw_points(key, part):
    total = ROWS_DEV * N_ROWS * N_GRP
    order = jax.random.permutation(jax.random.fold_in(key, 11), total)
    return order[:NPTS].astype(jnp.int32)


def level_of(own_key, extent, shards, least, largest):
    level, own = 1.0, jax.random.fold_in(own_key, 6)
    for position, blocks in shards:
        heights = jnp.exp(jax.random.uniform(jax.random.fold_in(own, position), (blocks,), jnp.float32, least / len(shards), largest / len(shards)))
        level = level * jnp.repeat(heights, extent[position] // blocks).reshape([-1 if axis == position else 1 for axis in range(len(extent))])
    return level


def gaussian(own_key, shape, spread, bound, split=(), kind=jnp.bfloat16):
    factor_of = level_of(own_key, shape, split, -0.22, 0.18) if split else 1.0
    result = jax.random.normal(own_key, shape, jnp.float32) * spread * factor_of
    return jnp.minimum(jnp.maximum(result, -bound), bound).astype(kind)


def setup_inputs(seed: int = 0) -> dict:
    seeds = jax.random.split(jax.random.key(seed), 3)
    modes = gaussian(seeds[0], (ROWS, MODES), 1.0, 6.0, ((0, 32),), jnp.float32)
    points = draw_points(jax.random.fold_in(seeds[2], 71), 0)
    return {"modes": modes, "points": points}


def reference(modes, points):
    high = lax.Precision.HIGHEST
    sampled = modes[points.astype(jnp.int32)]
    fit_modes = modes[:, :FIT]
    rest_modes = modes[:, FIT:]
    total = ROWS_DEV * N_ROWS * N_GRP
    collected = []
    residual = rest_modes
    for step in range(STEPS):
        chosen = sampled[:PRIOR + step + 1]
        left = chosen[:, :FIT]
        right = chosen[:, FIT:]
        gram = jnp.dot(left.T.astype(jnp.float32), left.astype(jnp.float32), preferred_element_type=jnp.float32, precision=high)
        cross = jnp.dot(left.T.astype(jnp.float32), right.astype(jnp.float32), preferred_element_type=jnp.float32, precision=high)
        factor = jnp.linalg.cholesky(gram)
        coef = jax.scipy.linalg.cho_solve((factor, True), cross)
        residual = rest_modes - jnp.dot(fit_modes.astype(jnp.float32), coef.astype(jnp.float32), preferred_element_type=jnp.float32, precision=high)
        collected.append(jnp.sum(residual * residual, axis=0) / total)
    return (residual, jnp.stack(collected))
```

```python
import functools

import jax
import jax.numpy as jnp
from jax import lax
from jax.experimental import pallas as pl
from jax.experimental.pallas import tpu as pltpu
from jax.sharding import PartitionSpec as P

PRIOR = 192
LANES = 128
HIGH = lax.Precision.HIGHEST
MESH = pl.DeviceIdType.MESH


def dot(a, b, dims=((1,), (0,))):
    return lax.dot_general(a, b, (dims, ((), ())), precision=HIGH, preferred_element_type=jnp.float32)


def flat_index(axes):
    (first, _), (second, width) = axes
    return lax.axis_index(first) * width + lax.axis_index(second)


def coords(axes, flat):
    width = axes[1][1]
    return (flat // width, lax.rem(flat, width))


def pick_kernel(axes, n, points_ref, modes_ref, out_ref, picked, sem):
    rows_dev, cols = modes_ref.shape
    npts = points_ref.shape[0]
    split = cols // 2
    base = flat_index(axes) * rows_dev
    picked[...] = jnp.zeros_like(picked)

    def row_copy(i):
        local = points_ref[i] - base
        owned = (local >= 0) & (local < rows_dev)
        safe = jnp.clip(local, 0, rows_dev - 1)
        return owned, pltpu.make_async_copy(
            modes_ref.at[pl.ds(safe, 1), :], picked.at[pl.ds(i, 1), :], sem
        )

    def issue(i, count):
        owned, copy = row_copy(i)

        @pl.when(owned)
        def _():
            copy.start()

        return count

    def drain(i, count):
        owned, copy = row_copy(i)

        @pl.when(owned)
        def _():
            copy.wait()

        return count

    lax.fori_loop(0, npts, issue, 0)
    lax.fori_loop(0, npts, drain, 0)
    block = picked[...]
    index = lax.broadcasted_iota(jnp.int32, block.shape, 0)
    chosen = jnp.where(index <= PRIOR, block, 0.0)
    both = dot(chosen[:, :split], chosen, ((0,), (0,)))
    rp = 2 * split // n
    for i in range(n):
        row, col = (i * rp) % split, (i * rp) // split * split
        out_ref[i, 0:rp, :] = both[row : row + rp, col : col + split]
    fresh = npts - PRIOR - 1
    out_ref[:, rp : rp + 1, :] = jnp.zeros((n, 1, split), jnp.float32)
    for i in range(fresh):
        for half in range(2):
            at = PRIOR + 1 + i
            out_ref[2 * i + half, rp : rp + 1, :] = picked[at : at + 1, half * split : (half + 1) * split]


def barrier_all(axes, n, me):
    barrier = pltpu.get_barrier_semaphore()

    def greet(off, carry):
        peer = lax.rem(me + off, n)
        pl.semaphore_signal(barrier, inc=1, device_id=coords(axes, peer), device_id_type=MESH)
        return carry

    lax.fori_loop(1, n, greet, 0)
    pl.semaphore_wait(barrier, n - 1)


def sweep_inverse(gram):
    size = gram.shape[0]
    tiles = [gram[8 * t : 8 * t + 8, :] for t in range(size // 8)]
    lane = lax.broadcasted_iota(jnp.int32, (8, size), 1)
    sub = lax.broadcasted_iota(jnp.int32, (8, size), 0)
    for k in range(size):
        t, s = k // 8, k % 8
        at_lane = lane == k
        row = jnp.broadcast_to(tiles[t][s : s + 1, :], (8, size))
        pivot = jnp.broadcast_to(row[:, k : k + 1], (8, size))
        inv = 1.0 / pivot
        scaled = jnp.where(at_lane, -inv, row * inv)
        fresh = []
        for r in range(size // 8):
            col = jnp.broadcast_to(tiles[r][:, k : k + 1], (8, size))
            fresh.append(jnp.where(at_lane, 0.0, tiles[r]) - col * scaled)
        fresh[t] = jnp.where(sub == s, scaled, fresh[t])
        tiles = fresh
    return -jnp.concatenate(tiles, axis=0)


def solve_kernel(axes, n, part_ref, hi_ref, lo_ref, landed, mine, full, square, send1, recv1, send2, recv2):
    me = flat_index(axes)
    rp = part_ref.shape[1] - 1
    split = part_ref.shape[2]
    barrier_all(axes, n, me)

    def scatter(off):
        peer = lax.rem(me + off, n)
        return pltpu.make_async_remote_copy(
            src_ref=part_ref.at[peer],
            dst_ref=landed.at[off],
            send_sem=send1.at[off],
            recv_sem=recv1.at[off],
            device_id=coords(axes, peer),
            device_id_type=MESH,
        )

    def spread(off):
        peer = lax.rem(me + off, n)
        return pltpu.make_async_remote_copy(
            src_ref=mine,
            dst_ref=full.at[me],
            send_sem=send2.at[off],
            recv_sem=recv2.at[off],
            device_id=coords(axes, peer),
            device_id_type=MESH,
        )

    def gathered(off):
        owner = lax.rem(me - off + n, n)
        return pltpu.make_async_remote_copy(
            src_ref=mine,
            dst_ref=full.at[owner],
            send_sem=send2.at[off],
            recv_sem=recv2.at[off],
            device_id=coords(axes, owner),
            device_id_type=MESH,
        )

    def loop(body):
        def step(off, carry):
            body(off)
            return carry

        lax.fori_loop(1, n, step, 0)

    loop(lambda off: scatter(off).start())
    loop(lambda off: scatter(off).wait_recv())
    total = part_ref[me]
    for off in range(1, n):
        total = total + landed[off]
    mine[...] = total
    full[me] = total
    loop(lambda off: scatter(off).wait_send())
    loop(lambda off: spread(off).start())
    loop(lambda off: gathered(off).wait_recv())
    loop(lambda off: spread(off).wait_send())

    for i in range(n):
        square[i * rp : (i + 1) * rp, :] = full[i, 0:rp, :]
    gram = square[0:split, :]
    cross = square[split : 2 * split, :]
    inverse = sweep_inverse(gram)
    coef = dot(inverse, cross)
    coef = coef + dot(inverse, cross - dot(gram, coef))
    left = [full[2 * i, rp : rp + 1, :] for i in range(3)]
    right = [full[2 * i + 1, rp : rp + 1, :] for i in range(3)]
    pad = jnp.zeros((5, split), jnp.float32)
    lefts = jnp.concatenate(left + [pad], axis=0)
    gains = dot(lefts, inverse)
    errors = dot(lefts, coef)
    kept = [coef]
    ks, ss, ds = [], [], []
    for j in range(3):
        k = gains[j : j + 1, :]
        d = right[j] - errors[j : j + 1, :]
        for k0, s0, d0 in zip(ks, ss, ds):
            along = jnp.sum(k0 * left[j], axis=1, keepdims=True)
            k = k - k0 * (along / s0)
            d = d - along * d0
        s = 1.0 + jnp.sum(k * left[j], axis=1, keepdims=True)
        d = d / s
        ks.append(k)
        ss.append(s)
        ds.append(d)
        pad7 = jnp.zeros((7, split), jnp.float32)
        coef = coef + dot(
            jnp.concatenate([k, pad7], axis=0), jnp.concatenate([d, pad7], axis=0), ((0,), (0,))
        )
        kept.append(coef)
    for j, value in enumerate(kept):
        hi = value.astype(jnp.bfloat16)
        hi_ref[:, j * split : (j + 1) * split] = hi
        lo_ref[:, j * split : (j + 1) * split] = (value - hi.astype(jnp.float32)).astype(jnp.bfloat16)


def residual_kernel(modes_ref, hi_ref, lo_ref, res_ref, sums_ref):
    split = res_ref.shape[1]
    steps = hi_ref.shape[1] // split
    fit = modes_ref[:, :split]
    rest = modes_ref[:, split:]
    hi = fit.astype(jnp.bfloat16)
    lo = (fit - hi.astype(jnp.float32)).astype(jnp.bfloat16)
    wide = jnp.concatenate([hi, lo], axis=1)
    top = hi_ref[...]
    f32 = jnp.float32
    made = jnp.dot(wide, jnp.concatenate([top, top], axis=0), preferred_element_type=f32)
    made = made + jnp.dot(hi, lo_ref[...], preferred_element_type=f32)

    @pl.when(pl.program_id(0) == 0)
    def _():
        sums_ref[...] = jnp.zeros_like(sums_ref)

    for j in range(steps):
        left = rest - made[:, j * split : (j + 1) * split]
        if j == steps - 1:
            res_ref[...] = left
        part = jnp.sum((left * left).reshape(-1, 8, split), axis=0)
        sums_ref[8 * j : 8 * j + 8, :] += part


def norm_kernel(axes, n, total_rows, sums_ref, out_ref, landed, mine, send, recv):
    me = flat_index(axes)
    steps = out_ref.shape[0]
    for j in range(steps):
        mine[j : j + 1, :] = jnp.sum(sums_ref[8 * j : 8 * j + 8, :], axis=0, keepdims=True)
    barrier_all(axes, n, me)

    def share(off):
        peer = lax.rem(me + off, n)
        return pltpu.make_async_remote_copy(
            src_ref=mine,
            dst_ref=landed.at[me],
            send_sem=send.at[off],
            recv_sem=recv.at[off],
            device_id=coords(axes, peer),
            device_id_type=MESH,
        )

    def arrival(off):
        owner = lax.rem(me - off + n, n)
        return pltpu.make_async_remote_copy(
            src_ref=mine,
            dst_ref=landed.at[owner],
            send_sem=send.at[off],
            recv_sem=recv.at[off],
            device_id=coords(axes, owner),
            device_id_type=MESH,
        )

    def loop(body):
        def step(off, carry):
            body(off)
            return carry

        lax.fori_loop(1, n, step, 0)

    loop(lambda off: share(off).start())
    landed[me] = mine[...]
    loop(lambda off: arrival(off).wait_recv())
    total = landed[0]
    for i in range(1, n):
        total = total + landed[i]
    out_ref[...] = total / total_rows
    loop(lambda off: share(off).wait_send())


def on_device(axes, modes, points):
    n = axes[0][1] * axes[1][1]
    rows_dev, cols = modes.shape
    split = cols // 2
    rp = 2 * split // n
    npts = points.shape[0]
    steps = npts - PRIOR
    padded = -(-npts // 8) * 8
    f32 = jnp.float32
    vmem = pl.BlockSpec(memory_space=pltpu.VMEM)
    part = pl.pallas_call(
        functools.partial(pick_kernel, axes, n),
        out_shape=jax.ShapeDtypeStruct((n, rp + 1, split), f32),
        in_specs=[pl.BlockSpec(memory_space=pltpu.SMEM), pl.BlockSpec(memory_space=pl.ANY)],
        out_specs=vmem,
        scratch_shapes=[pltpu.VMEM((padded, cols), f32), pltpu.SemaphoreType.DMA],
        name="pick",
    )(points, modes)
    hi, lo = pl.pallas_call(
        functools.partial(solve_kernel, axes, n),
        out_shape=[jax.ShapeDtypeStruct((split, steps * split), jnp.bfloat16)] * 2,
        in_specs=[vmem],
        out_specs=[vmem, vmem],
        scratch_shapes=[
            pltpu.VMEM((n, rp + 1, split), f32),
            pltpu.VMEM((rp + 1, split), f32),
            pltpu.VMEM((n, rp + 1, split), f32),
            pltpu.VMEM((2 * split, split), f32),
        ]
        + [pltpu.SemaphoreType.DMA((n,))] * 4,
        compiler_params=pltpu.CompilerParams(collective_id=0, has_side_effects=True),
        name="solve",
    )(part)
    tile = 2048 if rows_dev % 2048 == 0 else rows_dev
    residual, sums = pl.pallas_call(
        residual_kernel,
        grid=(rows_dev // tile,),
        out_shape=[jax.ShapeDtypeStruct((rows_dev, split), f32), jax.ShapeDtypeStruct((8 * steps, split), f32)],
        in_specs=[
            pl.BlockSpec((tile, cols), lambda i: (i, 0)),
            pl.BlockSpec((split, steps * split), lambda i: (0, 0)),
            pl.BlockSpec((split, steps * split), lambda i: (0, 0)),
        ],
        out_specs=[pl.BlockSpec((tile, split), lambda i: (i, 0)), pl.BlockSpec((8 * steps, split), lambda i: (0, 0))],
        name="residual",
    )(modes, hi, lo)
    norms = pl.pallas_call(
        functools.partial(norm_kernel, axes, n, rows_dev * n),
        out_shape=jax.ShapeDtypeStruct((steps, split), f32),
        in_specs=[vmem],
        out_specs=vmem,
        scratch_shapes=[
            pltpu.VMEM((n, steps, split), f32),
            pltpu.VMEM((steps, split), f32),
            pltpu.SemaphoreType.DMA((n,)),
            pltpu.SemaphoreType.DMA((n,)),
        ],
        compiler_params=pltpu.CompilerParams(collective_id=1, has_side_effects=True),
        name="norms",
    )(sums)
    return residual, norms


def solution(mesh):
    axes = tuple((name, mesh.shape[name]) for name in ("rows", "grp"))
    return jax.shard_map(
        functools.partial(on_device, axes),
        mesh=mesh,
        in_specs=(P(("rows", "grp"), None), P()),
        out_specs=(P(("rows", "grp"), None), P()),
        check_vma=False,
    )
```

```python
import functools

import jax
import jax.numpy as jnp
from jax import lax
from jax.experimental import pallas as pl
from jax.experimental.pallas import tpu as pltpu
from jax.sharding import PartitionSpec as P

PRIOR = 192
BLOCK = 8
HIGH = lax.Precision.HIGHEST
MESH = pl.DeviceIdType.MESH


def dot(a, b, dims=((1,), (0,))):
    return lax.dot_general(a, b, (dims, ((), ())), precision=HIGH, preferred_element_type=jnp.float32)


def flat_index(axes):
    (first, _), (second, width) = axes
    return lax.axis_index(first) * width + lax.axis_index(second)


def coords(axes, flat):
    width = axes[1][1]
    return (flat // width, lax.rem(flat, width))


def pick_kernel(axes, n, points_ref, modes_ref, out_ref, picked, sem):
    rows_dev, cols = modes_ref.shape
    npts = points_ref.shape[0]
    split = cols // 2
    base = flat_index(axes) * rows_dev
    picked[...] = jnp.zeros_like(picked)

    def row_copy(i):
        local = points_ref[i] - base
        owned = (local >= 0) & (local < rows_dev)
        safe = jnp.clip(local, 0, rows_dev - 1)
        return owned, pltpu.make_async_copy(
            modes_ref.at[pl.ds(safe, 1), :], picked.at[pl.ds(i, 1), :], sem
        )

    def issue(i, count):
        owned, copy = row_copy(i)

        @pl.when(owned)
        def _():
            copy.start()

        return count

    def drain(i, count):
        owned, copy = row_copy(i)

        @pl.when(owned)
        def _():
            copy.wait()

        return count

    lax.fori_loop(0, npts, issue, 0)
    lax.fori_loop(0, npts, drain, 0)
    block = picked[...]
    index = lax.broadcasted_iota(jnp.int32, block.shape, 0)
    chosen = jnp.where(index <= PRIOR, block, 0.0)
    both = dot(chosen[:, :split], chosen, ((0,), (0,)))
    rp = 2 * split // n
    for i in range(n):
        row, col = (i * rp) % split, (i * rp) // split * split
        out_ref[i, 0:rp, :] = both[row : row + rp, col : col + split]
    fresh = npts - PRIOR - 1
    out_ref[:, rp : rp + 1, :] = jnp.zeros((n, 1, split), jnp.float32)
    for i in range(fresh):
        for half in range(2):
            at = PRIOR + 1 + i
            out_ref[2 * i + half, rp : rp + 1, :] = picked[at : at + 1, half * split : (half + 1) * split]


def barrier_all(axes, n, me):
    barrier = pltpu.get_barrier_semaphore()

    def greet(off, carry):
        peer = lax.rem(me + off, n)
        pl.semaphore_signal(barrier, inc=1, device_id=coords(axes, peer), device_id_type=MESH)
        return carry

    lax.fori_loop(1, n, greet, 0)
    pl.semaphore_wait(barrier, n - 1)


def small_inverse(e):
    size = len(e)
    e = [list(line) for line in e]
    for p in range(size):
        inv = 1.0 / e[p][p]
        line = [e[p][j] * inv for j in range(size)]
        line[p] = -inv
        for i in range(size):
            for j in range(i, size):
                if i == p or j == p:
                    continue
                e[i][j] = e[i][j] - e[p][i] * line[j]
                e[j][i] = e[i][j]
        for j in range(size):
            e[p][j] = line[j]
            e[j][p] = line[j]
    return [[-value for value in line] for line in e]


def sweep_inverse(gram, width=BLOCK):
    size = gram.shape[0]
    shape = (8, size)
    tiles = [gram[8 * t : 8 * t + 8, :] for t in range(size // 8)]
    lane = lax.broadcasted_iota(jnp.int32, shape, 1)
    sub = lax.broadcasted_iota(jnp.int32, shape, 0)
    for k in range(0, size, width):
        t, s = k // 8, k % 8
        inside = (lane >= k) & (lane < k + width)
        own = [jnp.broadcast_to(tiles[t][:, k + q : k + q + 1], shape) for q in range(width)]
        entry = [[None] * width for _ in range(width)]
        for p in range(width):
            for q in range(p, width):
                entry[p][q] = jnp.broadcast_to(own[q][s + p : s + p + 1, :], shape)
                entry[q][p] = entry[p][q]
        small = small_inverse(entry)
        rows = []
        for q in range(width):
            row = jnp.broadcast_to(tiles[t][s + q : s + q + 1, :], shape)
            rows.append(jnp.where(inside, jnp.where(lane == k + q, -1.0, 0.0), row))
        scaled = []
        for p in range(width):
            line = small[p][0] * rows[0]
            for q in range(1, width):
                line = line + small[p][q] * rows[q]
            scaled.append(line)
        fresh = []
        for r in range(size // 8):
            value = jnp.where(inside, 0.0, tiles[r])
            for p in range(width):
                col = own[p] if r == t else jnp.broadcast_to(tiles[r][:, k + p : k + p + 1], shape)
                value = value - col * scaled[p]
            fresh.append(value)
        for p in range(width):
            fresh[t] = jnp.where(sub == s + p, scaled[p], fresh[t])
        tiles = fresh
    return -jnp.concatenate(tiles, axis=0)


def solve_kernel(axes, n, part_ref, wide_ref, delta_ref, landed, mine, full, square, send1, recv1, send2, recv2):
    me = flat_index(axes)
    rp = part_ref.shape[1] - 1
    split = part_ref.shape[2]
    barrier_all(axes, n, me)

    def scatter(off):
        peer = lax.rem(me + off, n)
        return pltpu.make_async_remote_copy(
            src_ref=part_ref.at[peer],
            dst_ref=landed.at[off],
            send_sem=send1.at[off],
            recv_sem=recv1.at[off],
            device_id=coords(axes, peer),
            device_id_type=MESH,
        )

    def spread(off):
        peer = lax.rem(me + off, n)
        return pltpu.make_async_remote_copy(
            src_ref=mine,
            dst_ref=full.at[me],
            send_sem=send2.at[off],
            recv_sem=recv2.at[off],
            device_id=coords(axes, peer),
            device_id_type=MESH,
        )

    def gathered(off):
        owner = lax.rem(me - off + n, n)
        return pltpu.make_async_remote_copy(
            src_ref=mine,
            dst_ref=full.at[owner],
            send_sem=send2.at[off],
            recv_sem=recv2.at[off],
            device_id=coords(axes, owner),
            device_id_type=MESH,
        )

    def loop(body):
        def step(off, carry):
            body(off)
            return carry

        lax.fori_loop(1, n, step, 0)

    loop(lambda off: scatter(off).start())
    loop(lambda off: scatter(off).wait_recv())
    total = part_ref[me]
    for off in range(1, n):
        total = total + landed[off]
    mine[...] = total
    full[me] = total
    loop(lambda off: scatter(off).wait_send())
    loop(lambda off: spread(off).start())
    loop(lambda off: gathered(off).wait_recv())
    loop(lambda off: spread(off).wait_send())

    for i in range(n):
        square[i * rp : (i + 1) * rp, :] = full[i, 0:rp, :]
    gram = square[0:split, :]
    cross = square[split : 2 * split, :]
    inverse = sweep_inverse(gram)
    coef = dot(inverse, cross)
    coef = coef + dot(inverse, cross - dot(gram, coef))
    left = [full[2 * i, rp : rp + 1, :] for i in range(3)]
    right = [full[2 * i + 1, rp : rp + 1, :] for i in range(3)]
    pad = jnp.zeros((5, split), jnp.float32)
    lefts = jnp.concatenate(left + [pad], axis=0)
    gains = dot(lefts, inverse)
    errors = dot(lefts, coef)
    ks, ss, ds = [], [], []
    for j in range(3):
        k = gains[j : j + 1, :]
        d = right[j] - errors[j : j + 1, :]
        for k0, s0, d0 in zip(ks, ss, ds):
            along = jnp.sum(k0 * left[j], axis=1, keepdims=True)
            k = k - k0 * (along / s0)
            d = d - along * d0
        s = 1.0 + jnp.sum(k * left[j], axis=1, keepdims=True)
        d = d / s
        ks.append(k)
        ss.append(s)
        ds.append(d)
    gain = jnp.concatenate(ks + [pad], axis=0)
    delta = jnp.concatenate(ds + [pad], axis=0)
    coef = coef + dot(gain, delta, ((0,), (0,)))
    delta_ref[...] = delta
    full_gain = jnp.transpose(jnp.concatenate([gain, jnp.zeros((split - 8, split), jnp.float32)], axis=0))
    zero = jnp.zeros((split, split), jnp.bfloat16)
    c_hi, c_lo = halves(coef)
    k_hi, k_lo = halves(full_gain)
    wide_ref[0:split, 0:split] = c_hi
    wide_ref[split:, 0:split] = c_hi
    wide_ref[0:split, split : 2 * split] = c_lo
    wide_ref[split:, split : 2 * split] = zero
    wide_ref[0:split, 2 * split : 3 * split] = k_hi
    wide_ref[split:, 2 * split : 3 * split] = k_hi
    wide_ref[0:split, 3 * split :] = k_lo
    wide_ref[split:, 3 * split :] = zero


def halves(value):
    hi = value.astype(jnp.bfloat16)
    return hi, (value - hi.astype(jnp.float32)).astype(jnp.bfloat16)


def residual_kernel(modes_ref, wide_ref, delta_ref, res_ref, sums_ref):
    split = res_ref.shape[1]
    steps = sums_ref.shape[0] // 8

    @pl.when(pl.program_id(0) == 0)
    def _():
        sums_ref[...] = jnp.zeros_like(sums_ref)

    rows = res_ref.shape[0]
    chunk = 256 if rows % 256 == 0 else rows
    wide = wide_ref[...]
    deltas = [delta_ref[j : j + 1, :] for j in range(steps - 1)]
    totals = [sums_ref[8 * j : 8 * j + 8, :] for j in range(steps)]
    for at in range(0, rows, chunk):
        hi, lo = halves(modes_ref[at : at + chunk, :split])
        pair = jnp.concatenate([hi, lo], axis=1)
        made = jnp.dot(pair, wide, preferred_element_type=jnp.float32)
        left = modes_ref[at : at + chunk, split:] - (made[:, :split] + made[:, split : 2 * split])
        res_ref[at : at + chunk, :] = left
        along = made[:, 2 * split : 3 * split] + made[:, 3 * split :]
        for j in range(steps - 1, -1, -1):
            totals[j] = totals[j] + jnp.sum((left * left).reshape(-1, 8, split), axis=0)
            if j:
                left = left + along[:, j - 1 : j] * deltas[j - 1]
    for j in range(steps):
        sums_ref[8 * j : 8 * j + 8, :] = totals[j]


def norm_kernel(axes, n, total_rows, sums_ref, out_ref, landed, mine, send, recv):
    me = flat_index(axes)
    steps = out_ref.shape[0]
    for j in range(steps):
        mine[j : j + 1, :] = jnp.sum(sums_ref[8 * j : 8 * j + 8, :], axis=0, keepdims=True)
    barrier_all(axes, n, me)

    def share(off):
        peer = lax.rem(me + off, n)
        return pltpu.make_async_remote_copy(
            src_ref=mine,
            dst_ref=landed.at[me],
            send_sem=send.at[off],
            recv_sem=recv.at[off],
            device_id=coords(axes, peer),
            device_id_type=MESH,
        )

    def arrival(off):
        owner = lax.rem(me - off + n, n)
        return pltpu.make_async_remote_copy(
            src_ref=mine,
            dst_ref=landed.at[owner],
            send_sem=send.at[off],
            recv_sem=recv.at[off],
            device_id=coords(axes, owner),
            device_id_type=MESH,
        )

    def loop(body):
        def step(off, carry):
            body(off)
            return carry

        lax.fori_loop(1, n, step, 0)

    loop(lambda off: share(off).start())
    landed[me] = mine[...]
    loop(lambda off: arrival(off).wait_recv())
    total = landed[0]
    for i in range(1, n):
        total = total + landed[i]
    out_ref[...] = total / total_rows
    loop(lambda off: share(off).wait_send())


def on_device(axes, modes, points):
    n = axes[0][1] * axes[1][1]
    rows_dev, cols = modes.shape
    split = cols // 2
    rp = 2 * split // n
    npts = points.shape[0]
    steps = npts - PRIOR
    padded = -(-npts // 8) * 8
    f32 = jnp.float32
    vmem = pl.BlockSpec(memory_space=pltpu.VMEM)
    part = pl.pallas_call(
        functools.partial(pick_kernel, axes, n),
        out_shape=jax.ShapeDtypeStruct((n, rp + 1, split), f32),
        in_specs=[pl.BlockSpec(memory_space=pltpu.SMEM), pl.BlockSpec(memory_space=pl.ANY)],
        out_specs=vmem,
        scratch_shapes=[pltpu.VMEM((padded, cols), f32), pltpu.SemaphoreType.DMA],
        name="pick",
    )(points, modes)
    wide, delta = pl.pallas_call(
        functools.partial(solve_kernel, axes, n),
        out_shape=[jax.ShapeDtypeStruct((2 * split, 4 * split), jnp.bfloat16), jax.ShapeDtypeStruct((8, split), f32)],
        in_specs=[vmem],
        out_specs=[vmem, vmem],
        scratch_shapes=[
            pltpu.VMEM((n, rp + 1, split), f32),
            pltpu.VMEM((rp + 1, split), f32),
            pltpu.VMEM((n, rp + 1, split), f32),
            pltpu.VMEM((2 * split, split), f32),
        ]
        + [pltpu.SemaphoreType.DMA((n,))] * 4,
        compiler_params=pltpu.CompilerParams(collective_id=0, has_side_effects=True),
        name="solve",
    )(part)
    tile = 2048 if rows_dev % 2048 == 0 else rows_dev
    residual, sums = pl.pallas_call(
        residual_kernel,
        grid=(rows_dev // tile,),
        out_shape=[jax.ShapeDtypeStruct((rows_dev, split), f32), jax.ShapeDtypeStruct((8 * steps, split), f32)],
        in_specs=[
            pl.BlockSpec((tile, cols), lambda i: (i, 0)),
            pl.BlockSpec((2 * split, 4 * split), lambda i: (0, 0)),
            pl.BlockSpec((8, split), lambda i: (0, 0)),
        ],
        out_specs=[pl.BlockSpec((tile, split), lambda i: (i, 0)), pl.BlockSpec((8 * steps, split), lambda i: (0, 0))],
        name="residual",
    )(modes, wide, delta)
    norms = pl.pallas_call(
        functools.partial(norm_kernel, axes, n, rows_dev * n),
        out_shape=jax.ShapeDtypeStruct((steps, split), f32),
        in_specs=[vmem],
        out_specs=vmem,
        scratch_shapes=[
            pltpu.VMEM((n, steps, split), f32),
            pltpu.VMEM((steps, split), f32),
            pltpu.SemaphoreType.DMA((n,)),
            pltpu.SemaphoreType.DMA((n,)),
        ],
        compiler_params=pltpu.CompilerParams(collective_id=1, has_side_effects=True),
        name="norms",
    )(sums)
    return residual, norms


def solution(mesh):
    axes = tuple((name, mesh.shape[name]) for name in ("rows", "grp"))
    return jax.shard_map(
        functools.partial(on_device, axes),
        mesh=mesh,
        in_specs=(P(("rows", "grp"), None), P()),
        out_specs=(P(("rows", "grp"), None), P()),
        check_vma=False,
    )
```

```python
import functools

import jax
import jax.numpy as jnp
from jax import lax
from jax.experimental import pallas as pl
from jax.experimental.pallas import tpu as pltpu
from jax.sharding import PartitionSpec as P

PRIOR = 192
BLOCK = 8
HOOK_AT = 80
FIRST, SECOND = 4, 8
HIGH = lax.Precision.HIGHEST
MESH = pl.DeviceIdType.MESH


def dot(a, b, dims=((1,), (0,))):
    return lax.dot_general(a, b, (dims, ((), ())), precision=HIGH, preferred_element_type=jnp.float32)


def flat_index(axes):
    (first, _), (second, width) = axes
    return lax.axis_index(first) * width + lax.axis_index(second)


def coords(axes, flat):
    width = axes[1][1]
    return (flat // width, lax.rem(flat, width))


def pick_kernel(axes, n, points_ref, modes_ref, out_ref, picked, sem):
    rows_dev, cols = modes_ref.shape
    npts = points_ref.shape[0]
    split = cols // 2
    base = flat_index(axes) * rows_dev
    picked[...] = jnp.zeros_like(picked)

    def row_copy(i):
        local = points_ref[i] - base
        owned = (local >= 0) & (local < rows_dev)
        safe = jnp.clip(local, 0, rows_dev - 1)
        return owned, pltpu.make_async_copy(
            modes_ref.at[pl.ds(safe, 1), :], picked.at[pl.ds(i, 1), :], sem
        )

    def issue(i, count):
        owned, copy = row_copy(i)

        @pl.when(owned)
        def _():
            copy.start()

        return count

    def drain(i, count):
        owned, copy = row_copy(i)

        @pl.when(owned)
        def _():
            copy.wait()

        return count

    lax.fori_loop(0, npts, issue, 0)
    lax.fori_loop(0, npts, drain, 0)
    block = picked[...]
    index = lax.broadcasted_iota(jnp.int32, block.shape, 0)
    chosen = jnp.where(index <= PRIOR, block, 0.0)
    both = dot(chosen[:, :split], chosen, ((0,), (0,)))
    rp = 2 * split // n
    for i in range(n):
        row, col = (i * rp) % split, (i * rp) // split * split
        out_ref[i, 0:rp, :] = both[row : row + rp, col : col + split]
    fresh = npts - PRIOR - 1
    out_ref[:, rp : rp + 1, :] = jnp.zeros((n, 1, split), jnp.float32)
    for i in range(fresh):
        for half in range(2):
            at = PRIOR + 1 + i
            out_ref[2 * i + half, rp : rp + 1, :] = picked[at : at + 1, half * split : (half + 1) * split]


def barrier_all(axes, n, me):
    barrier = pltpu.get_barrier_semaphore()

    def greet(off, carry):
        peer = lax.rem(me + off, n)
        pl.semaphore_signal(barrier, inc=1, device_id=coords(axes, peer), device_id_type=MESH)
        return carry

    lax.fori_loop(1, n, greet, 0)
    pl.semaphore_wait(barrier, n - 1)


def small_inverse(e):
    size = len(e)
    e = [list(line) for line in e]
    for p in range(size):
        inv = 1.0 / e[p][p]
        line = [e[p][j] * inv for j in range(size)]
        line[p] = -inv
        for i in range(size):
            for j in range(i, size):
                if i == p or j == p:
                    continue
                e[i][j] = e[i][j] - e[p][i] * line[j]
                e[j][i] = e[i][j]
        for j in range(size):
            e[p][j] = line[j]
            e[j][p] = line[j]
    return [[-value for value in line] for line in e]


def sweep_inverse(gram, hook, width=BLOCK):
    size = gram.shape[0]
    shape = (8, size)
    tiles = [gram[8 * t : 8 * t + 8, :] for t in range(size // 8)]
    lane = lax.broadcasted_iota(jnp.int32, shape, 1)
    sub = lax.broadcasted_iota(jnp.int32, shape, 0)
    for k in range(0, size, width):
        if k == HOOK_AT:
            hook()
        t, s = k // 8, k % 8
        inside = (lane >= k) & (lane < k + width)
        own = [jnp.broadcast_to(tiles[t][:, k + q : k + q + 1], shape) for q in range(width)]
        entry = [[None] * width for _ in range(width)]
        for p in range(width):
            for q in range(p, width):
                entry[p][q] = jnp.broadcast_to(own[q][s + p : s + p + 1, :], shape)
                entry[q][p] = entry[p][q]
        small = small_inverse(entry)
        rows = []
        for q in range(width):
            row = jnp.broadcast_to(tiles[t][s + q : s + q + 1, :], shape)
            rows.append(jnp.where(inside, jnp.where(lane == k + q, -1.0, 0.0), row))
        scaled = []
        for p in range(width):
            line = small[p][0] * rows[0]
            for q in range(1, width):
                line = line + small[p][q] * rows[q]
            scaled.append(line)
        fresh = []
        for r in range(size // 8):
            value = jnp.where(inside, 0.0, tiles[r])
            for p in range(width):
                col = own[p] if r == t else jnp.broadcast_to(tiles[r][:, k + p : k + p + 1], shape)
                value = value - col * scaled[p]
            fresh.append(value)
        for p in range(width):
            fresh[t] = jnp.where(sub == s + p, scaled[p], fresh[t])
        tiles = fresh
    return -jnp.concatenate(tiles, axis=0)


def solve_kernel(
    axes, n, part_ref, modes_ref, wide_ref, norm_ref,
    landed, mine, full, part2, landed2, mine2, full2, square, held, acc, squares,
    send1, recv1, send2, recv2, local,
):
    me = flat_index(axes)
    rp = part_ref.shape[1] - 1
    split = part_ref.shape[2]
    steps = norm_ref.shape[0]
    chunks, rows = held.shape[0], held.shape[1]
    total_rows = chunks * rows * n

    def loop(body, first=1, last=n):
        def step(off, carry):
            body(off)
            return carry

        lax.fori_loop(first, last, step, 0)

    def fetch(c):
        return pltpu.make_async_copy(
            modes_ref.at[pl.ds(c * rows, rows), :], held.at[c], local.at[c]
        )

    loop(lambda c: fetch(c).start(), 0, chunks)
    barrier = pltpu.get_barrier_semaphore()

    def greet(off):
        peer = lax.rem(me + off, n)
        pl.semaphore_signal(barrier, inc=1, device_id=coords(axes, peer), device_id_type=MESH)

    loop(greet)
    acc[...] = jnp.zeros_like(acc)
    squares[...] = jnp.zeros_like(squares)

    def grams(c):
        fetch(c).wait()
        acc[...] += dot(held[c, :, :split], held[c], ((0,), (0,)))
        rest = held[c, :, split:]
        squares[...] += jnp.sum((rest * rest).reshape(-1, 8, split), axis=0)

    def scatter(src, dst, off):
        peer = lax.rem(me + off, n)
        return pltpu.make_async_remote_copy(
            src_ref=src.at[peer],
            dst_ref=dst.at[off],
            send_sem=send1.at[off],
            recv_sem=recv1.at[off],
            device_id=coords(axes, peer),
            device_id_type=MESH,
        )

    def spread(src, dst, off):
        peer = lax.rem(me + off, n)
        return pltpu.make_async_remote_copy(
            src_ref=src,
            dst_ref=dst.at[me],
            send_sem=send2.at[off],
            recv_sem=recv2.at[off],
            device_id=coords(axes, peer),
            device_id_type=MESH,
        )

    def gathered(src, dst, off):
        owner = lax.rem(me - off + n, n)
        return pltpu.make_async_remote_copy(
            src_ref=src,
            dst_ref=dst.at[owner],
            send_sem=send2.at[off],
            recv_sem=recv2.at[off],
            device_id=coords(axes, owner),
            device_id_type=MESH,
        )

    def reduced(src, got, own, whole):
        loop(lambda off: scatter(src, got, off).wait_recv())
        total = src[me]
        for off in range(1, n):
            total = total + got[off]
        own[...] = total
        whole[me] = total
        loop(lambda off: scatter(src, got, off).wait_send())
        loop(lambda off: spread(own, whole, off).start())

    def finish(own, whole):
        loop(lambda off: gathered(own, whole, off).wait_recv())
        loop(lambda off: spread(own, whole, off).wait_send())
        for i in range(n):
            square[i * rp : (i + 1) * rp, :] = whole[i, 0:rp, :]
        return square[0:split, :], square[split : 2 * split, :]

    first, second = min(FIRST, chunks), min(SECOND, chunks)
    pl.semaphore_wait(barrier, n - 1)
    loop(lambda off: scatter(part_ref, landed, off).start())
    loop(grams, 0, first)
    reduced(part_ref, landed, mine, full)
    loop(grams, first, chunks)
    part2[...] = jnp.zeros_like(part2)
    for i in range(n):
        row, col = (i * rp) % split, (i * rp) // split * split
        part2[i, 0:rp, :] = acc[row : row + rp, col : col + split]
    part2[0, rp : rp + 1, :] = jnp.sum(squares[...], axis=0, keepdims=True)
    gram, cross = finish(mine, full)
    loop(lambda off: scatter(part2, landed2, off).start())
    inverse = sweep_inverse(gram, lambda: reduced(part2, landed2, mine2, full2))
    coef = dot(inverse, cross)
    coef = coef + dot(inverse, cross - dot(gram, coef))
    left = [full[2 * i, rp : rp + 1, :] for i in range(3)]
    right = [full[2 * i + 1, rp : rp + 1, :] for i in range(3)]
    pad = jnp.zeros((5, split), jnp.float32)
    lefts = jnp.concatenate(left + [pad], axis=0)
    gains = dot(lefts, inverse)
    errors = dot(lefts, coef)
    ks, ss, ds = [], [], []
    kept = [coef]
    pad7 = jnp.zeros((7, split), jnp.float32)
    for j in range(3):
        k = gains[j : j + 1, :]
        d = right[j] - errors[j : j + 1, :]
        for k0, s0, d0 in zip(ks, ss, ds):
            along = jnp.sum(k0 * left[j], axis=1, keepdims=True)
            k = k - k0 * (along / s0)
            d = d - along * d0
        s = 1.0 + jnp.sum(k * left[j], axis=1, keepdims=True)
        d = d / s
        ks.append(k)
        ss.append(s)
        ds.append(d)
        turn = dot(jnp.concatenate([k, pad7], axis=0), jnp.concatenate([d, pad7], axis=0), ((0,), (0,)))
        kept.append(kept[-1] + turn)
    c_hi, c_lo = halves(kept[-1])
    wide_ref[0:split, 0:split] = c_hi
    wide_ref[split:, 0:split] = c_hi
    wide_ref[0:split, split : 2 * split] = c_lo
    wide_ref[split:, split : 2 * split] = jnp.zeros((split, split), jnp.bfloat16)
    ftf, ftr = finish(mine2, full2)
    sq = full2[0, rp : rp + 1, :]
    curved = dot(ftf, jnp.concatenate(kept, axis=1))
    for j in range(steps):
        bent = kept[j] * (curved[:, j * split : (j + 1) * split] - 2.0 * ftr)
        norm_ref[j : j + 1, :] = (sq + jnp.sum(bent, axis=0, keepdims=True)) / total_rows


def halves(value):
    hi = value.astype(jnp.bfloat16)
    return hi, (value - hi.astype(jnp.float32)).astype(jnp.bfloat16)


def residual_kernel(modes_ref, wide_ref, res_ref):
    rows, split = res_ref.shape
    chunk = 256 if rows % 256 == 0 else rows
    wide = wide_ref[...]
    for at in range(0, rows, chunk):
        hi, lo = halves(modes_ref[at : at + chunk, :split])
        pair = jnp.concatenate([hi, lo], axis=1)
        made = jnp.dot(pair, wide, preferred_element_type=jnp.float32)
        res_ref[at : at + chunk, :] = modes_ref[at : at + chunk, split:] - (made[:, :split] + made[:, split:])


def on_device(axes, modes, points):
    n = axes[0][1] * axes[1][1]
    rows_dev, cols = modes.shape
    split = cols // 2
    rp = 2 * split // n
    npts = points.shape[0]
    steps = npts - PRIOR
    padded = -(-npts // 8) * 8
    f32 = jnp.float32
    vmem = pl.BlockSpec(memory_space=pltpu.VMEM)
    part = pl.pallas_call(
        functools.partial(pick_kernel, axes, n),
        out_shape=jax.ShapeDtypeStruct((n, rp + 1, split), f32),
        in_specs=[pl.BlockSpec(memory_space=pltpu.SMEM), pl.BlockSpec(memory_space=pl.ANY)],
        out_specs=vmem,
        scratch_shapes=[pltpu.VMEM((padded, cols), f32), pltpu.SemaphoreType.DMA],
        name="pick",
    )(points, modes)
    chunks = 12 if rows_dev % 96 == 0 else 1
    chunk_shape = pltpu.VMEM((n, rp + 1, split), f32)
    own_shape = pltpu.VMEM((rp + 1, split), f32)
    wide, norms = pl.pallas_call(
        functools.partial(solve_kernel, axes, n),
        out_shape=[
            jax.ShapeDtypeStruct((2 * split, 2 * split), jnp.bfloat16),
            jax.ShapeDtypeStruct((steps, split), f32),
        ],
        in_specs=[vmem, pl.BlockSpec(memory_space=pl.ANY)],
        out_specs=[vmem, vmem],
        scratch_shapes=[
            chunk_shape,
            own_shape,
            chunk_shape,
            chunk_shape,
            chunk_shape,
            own_shape,
            chunk_shape,
            pltpu.VMEM((2 * split, split), f32),
            pltpu.VMEM((chunks, rows_dev // chunks, cols), f32),
            pltpu.VMEM((split, cols), f32),
            pltpu.VMEM((8, split), f32),
        ]
        + [pltpu.SemaphoreType.DMA((n,))] * 4
        + [pltpu.SemaphoreType.DMA((chunks,))],
        compiler_params=pltpu.CompilerParams(collective_id=0, has_side_effects=True),
        name="solve",
    )(part, modes)
    tile = 2048 if rows_dev % 2048 == 0 else rows_dev
    residual = pl.pallas_call(
        residual_kernel,
        grid=(rows_dev // tile,),
        out_shape=jax.ShapeDtypeStruct((rows_dev, split), f32),
        in_specs=[
            pl.BlockSpec((tile, cols), lambda i: (i, 0)),
            pl.BlockSpec((2 * split, 2 * split), lambda i: (0, 0)),
        ],
        out_specs=pl.BlockSpec((tile, split), lambda i: (i, 0)),
        name="residual",
    )(modes, wide)
    return residual, norms


def solution(mesh):
    axes = tuple((name, mesh.shape[name]) for name in ("rows", "grp"))
    return jax.shard_map(
        functools.partial(on_device, axes),
        mesh=mesh,
        in_specs=(P(("rows", "grp"), None), P()),
        out_specs=(P(("rows", "grp"), None), P()),
        check_vma=False,
    )
```

```python
import functools

import jax
import jax.numpy as jnp
from jax import lax
from jax.experimental import pallas as pl
from jax.experimental.pallas import tpu as pltpu
from jax.sharding import PartitionSpec as P

PRIOR = 192
BLOCK = 8
HOOK_AT = 80
EARLY, FIRST = 2, 6
HIGH = lax.Precision.HIGHEST
MESH = pl.DeviceIdType.MESH


def dot(a, b, dims=((1,), (0,))):
    return lax.dot_general(a, b, (dims, ((), ())), precision=HIGH, preferred_element_type=jnp.float32)


def flat_index(axes):
    (first, _), (second, width) = axes
    return lax.axis_index(first) * width + lax.axis_index(second)


def coords(axes, flat):
    width = axes[1][1]
    return (flat // width, lax.rem(flat, width))


def pick_kernel(axes, n, points_ref, modes_ref, out_ref, picked, sem):
    rows_dev, cols = modes_ref.shape
    npts = points_ref.shape[0]
    split = cols // 2
    base = flat_index(axes) * rows_dev
    picked[...] = jnp.zeros_like(picked)

    def row_copy(i):
        local = points_ref[i] - base
        owned = (local >= 0) & (local < rows_dev)
        safe = jnp.clip(local, 0, rows_dev - 1)
        return owned, pltpu.make_async_copy(
            modes_ref.at[pl.ds(safe, 1), :], picked.at[pl.ds(i, 1), :], sem
        )

    def issue(i, count):
        owned, copy = row_copy(i)

        @pl.when(owned)
        def _():
            copy.start()

        return count

    def drain(i, count):
        owned, copy = row_copy(i)

        @pl.when(owned)
        def _():
            copy.wait()

        return count

    lax.fori_loop(0, npts, issue, 0, unroll=4)
    lax.fori_loop(0, npts, drain, 0, unroll=4)
    block = picked[...]
    index = lax.broadcasted_iota(jnp.int32, block.shape, 0)
    chosen = jnp.where(index <= PRIOR, block, 0.0)
    both = dot(chosen[:, :split], chosen, ((0,), (0,)))
    rp = 2 * split // n
    for i in range(n):
        row, col = (i * rp) % split, (i * rp) // split * split
        out_ref[i, 0:rp, :] = both[row : row + rp, col : col + split]
    fresh = npts - PRIOR - 1
    out_ref[:, rp : rp + 1, :] = jnp.zeros((n, 1, split), jnp.float32)
    for i in range(fresh):
        for half in range(2):
            at = PRIOR + 1 + i
            out_ref[2 * i + half, rp : rp + 1, :] = picked[at : at + 1, half * split : (half + 1) * split]


def barrier_all(axes, n, me):
    barrier = pltpu.get_barrier_semaphore()

    def greet(off, carry):
        peer = lax.rem(me + off, n)
        pl.semaphore_signal(barrier, inc=1, device_id=coords(axes, peer), device_id_type=MESH)
        return carry

    lax.fori_loop(1, n, greet, 0)
    pl.semaphore_wait(barrier, n - 1)


def small_inverse(e):
    size = len(e)
    e = [list(line) for line in e]
    for p in range(size):
        inv = 1.0 / e[p][p]
        line = [e[p][j] * inv for j in range(size)]
        line[p] = -inv
        for i in range(size):
            for j in range(i, size):
                if i == p or j == p:
                    continue
                e[i][j] = e[i][j] - e[p][i] * line[j]
                e[j][i] = e[i][j]
        for j in range(size):
            e[p][j] = line[j]
            e[j][p] = line[j]
    return [[-value for value in line] for line in e]


def sweep_inverse(gram, hook, width=BLOCK):
    size = gram.shape[0]
    shape = (8, size)
    tiles = [gram[8 * t : 8 * t + 8, :] for t in range(size // 8)]
    lane = lax.broadcasted_iota(jnp.int32, shape, 1)
    sub = lax.broadcasted_iota(jnp.int32, shape, 0)
    for k in range(0, size, width):
        if k == HOOK_AT:
            hook()
        t, s = k // 8, k % 8
        inside = (lane >= k) & (lane < k + width)
        own = [jnp.broadcast_to(tiles[t][:, k + q : k + q + 1], shape) for q in range(width)]
        entry = [[None] * width for _ in range(width)]
        for p in range(width):
            for q in range(p, width):
                entry[p][q] = jnp.broadcast_to(own[q][s + p : s + p + 1, :], shape)
                entry[q][p] = entry[p][q]
        small = small_inverse(entry)
        rows = []
        for q in range(width):
            row = jnp.broadcast_to(tiles[t][s + q : s + q + 1, :], shape)
            rows.append(jnp.where(inside, jnp.where(lane == k + q, -1.0, 0.0), row))
        scaled = []
        for p in range(width):
            line = small[p][0] * rows[0]
            for q in range(1, width):
                line = line + small[p][q] * rows[q]
            scaled.append(line)
        fresh = []
        for r in range(size // 8):
            value = jnp.where(inside, 0.0, tiles[r])
            for p in range(width):
                col = own[p] if r == t else jnp.broadcast_to(tiles[r][:, k + p : k + p + 1], shape)
                value = value - col * scaled[p]
            fresh.append(value)
        for p in range(width):
            fresh[t] = jnp.where(sub == s + p, scaled[p], fresh[t])
        tiles = fresh
    return -jnp.concatenate(tiles, axis=0)


def solve_kernel(
    axes, n, part_ref, modes_ref, wide_ref, norm_ref,
    landed, mine, full, part2, landed2, mine2, full2, square, held, acc, squares,
    send1, recv1, send2, recv2, local,
):
    me = flat_index(axes)
    rp = part_ref.shape[1] - 1
    split = part_ref.shape[2]
    steps = norm_ref.shape[0]
    chunks, rows = held.shape[0], held.shape[1]
    total_rows = chunks * rows * n

    def loop(body, first=1, last=n):
        def step(off, carry):
            body(off)
            return carry

        lax.fori_loop(first, last, step, 0)

    def fetch(c):
        return pltpu.make_async_copy(
            modes_ref.at[pl.ds(c * rows, rows), :], held.at[c], local.at[c]
        )

    loop(lambda c: fetch(c).start(), 0, chunks)
    barrier = pltpu.get_barrier_semaphore()

    def greet(off):
        peer = lax.rem(me + off, n)
        pl.semaphore_signal(barrier, inc=1, device_id=coords(axes, peer), device_id_type=MESH)

    loop(greet)
    acc[...] = jnp.zeros_like(acc)
    squares[...] = jnp.zeros_like(squares)

    def grams(c):
        fetch(c).wait()
        acc[...] += dot(held[c, :, :split], held[c], ((0,), (0,)))
        rest = held[c, :, split:]
        squares[...] += jnp.sum((rest * rest).reshape(-1, 8, split), axis=0)

    def scatter(src, dst, off):
        peer = lax.rem(me + off, n)
        return pltpu.make_async_remote_copy(
            src_ref=src.at[peer],
            dst_ref=dst.at[off],
            send_sem=send1.at[off],
            recv_sem=recv1.at[off],
            device_id=coords(axes, peer),
            device_id_type=MESH,
        )

    def spread(src, dst, off):
        peer = lax.rem(me + off, n)
        return pltpu.make_async_remote_copy(
            src_ref=src,
            dst_ref=dst.at[me],
            send_sem=send2.at[off],
            recv_sem=recv2.at[off],
            device_id=coords(axes, peer),
            device_id_type=MESH,
        )

    def gathered(src, dst, off):
        owner = lax.rem(me - off + n, n)
        return pltpu.make_async_remote_copy(
            src_ref=src,
            dst_ref=dst.at[owner],
            send_sem=send2.at[off],
            recv_sem=recv2.at[off],
            device_id=coords(axes, owner),
            device_id_type=MESH,
        )

    def reduced(src, got, own, whole):
        loop(lambda off: scatter(src, got, off).wait_recv())
        total = src[me]
        for off in range(1, n):
            total = total + got[off]
        own[...] = total
        whole[me] = total
        loop(lambda off: scatter(src, got, off).wait_send())
        loop(lambda off: spread(own, whole, off).start())

    def finish(own, whole):
        loop(lambda off: gathered(own, whole, off).wait_recv())
        loop(lambda off: spread(own, whole, off).wait_send())
        for i in range(n):
            square[i * rp : (i + 1) * rp, :] = whole[i, 0:rp, :]
        return square[0:split, :], square[split : 2 * split, :]

    early, first = min(EARLY, chunks), min(FIRST, chunks)
    loop(grams, 0, early)
    pl.semaphore_wait(barrier, n - 1)
    loop(lambda off: scatter(part_ref, landed, off).start())
    loop(grams, early, first)
    reduced(part_ref, landed, mine, full)
    loop(grams, first, chunks)
    part2[...] = jnp.zeros_like(part2)
    for i in range(n):
        row, col = (i * rp) % split, (i * rp) // split * split
        part2[i, 0:rp, :] = acc[row : row + rp, col : col + split]
    part2[0, rp : rp + 1, :] = jnp.sum(squares[...], axis=0, keepdims=True)
    gram, cross = finish(mine, full)
    loop(lambda off: scatter(part2, landed2, off).start())
    inverse = sweep_inverse(gram, lambda: reduced(part2, landed2, mine2, full2))
    coef = dot(inverse, cross)
    coef = coef + dot(inverse, cross - dot(gram, coef))
    left = [full[2 * i, rp : rp + 1, :] for i in range(3)]
    right = [full[2 * i + 1, rp : rp + 1, :] for i in range(3)]
    pad = jnp.zeros((5, split), jnp.float32)
    lefts = jnp.concatenate(left + [pad], axis=0)
    gains = dot(lefts, inverse)
    errors = dot(lefts, coef)
    ks, ss, ds = [], [], []
    kept = [coef]
    pad7 = jnp.zeros((7, split), jnp.float32)
    for j in range(3):
        k = gains[j : j + 1, :]
        d = right[j] - errors[j : j + 1, :]
        for k0, s0, d0 in zip(ks, ss, ds):
            along = jnp.sum(k0 * left[j], axis=1, keepdims=True)
            k = k - k0 * (along / s0)
            d = d - along * d0
        s = 1.0 + jnp.sum(k * left[j], axis=1, keepdims=True)
        d = d / s
        ks.append(k)
        ss.append(s)
        ds.append(d)
        turn = dot(jnp.concatenate([k, pad7], axis=0), jnp.concatenate([d, pad7], axis=0), ((0,), (0,)))
        kept.append(kept[-1] + turn)
    c_hi, c_lo = halves(kept[-1])
    wide_ref[0:split, 0:split] = c_hi
    wide_ref[split:, 0:split] = c_hi
    wide_ref[0:split, split : 2 * split] = c_lo
    wide_ref[split:, split : 2 * split] = jnp.zeros((split, split), jnp.bfloat16)
    ftf, ftr = finish(mine2, full2)
    sq = full2[0, rp : rp + 1, :]
    curved = dot(ftf, jnp.concatenate(kept, axis=1))
    for j in range(steps):
        bent = kept[j] * (curved[:, j * split : (j + 1) * split] - 2.0 * ftr)
        norm_ref[j : j + 1, :] = (sq + jnp.sum(bent, axis=0, keepdims=True)) / total_rows


def halves(value):
    hi = value.astype(jnp.bfloat16)
    return hi, (value - hi.astype(jnp.float32)).astype(jnp.bfloat16)


def residual_kernel(modes_ref, wide_ref, res_ref, held, made_buf, read, wrote):
    chunks, rows, split = made_buf.shape
    piece = 256 if rows % 256 == 0 else rows

    def fetch(c):
        return pltpu.make_async_copy(modes_ref.at[pl.ds(c * rows, rows), :], held.at[c], read.at[c])

    def flush(c):
        return pltpu.make_async_copy(made_buf.at[c], res_ref.at[pl.ds(c * rows, rows), :], wrote.at[c])

    for c in range(chunks):
        fetch(c).start()
    wide = wide_ref[...]
    for c in range(chunks):
        fetch(c).wait()
        for at in range(0, rows, piece):
            hi, lo = halves(held[c, at : at + piece, :split])
            pair = jnp.concatenate([hi, lo], axis=1)
            made = jnp.dot(pair, wide, preferred_element_type=jnp.float32)
            made_buf[c, at : at + piece, :] = held[c, at : at + piece, split:] - (made[:, :split] + made[:, split:])
        flush(c).start()
    for c in range(chunks):
        flush(c).wait()


def on_device(axes, modes, points):
    n = axes[0][1] * axes[1][1]
    rows_dev, cols = modes.shape
    split = cols // 2
    rp = 2 * split // n
    npts = points.shape[0]
    steps = npts - PRIOR
    padded = -(-npts // 8) * 8
    f32 = jnp.float32
    vmem = pl.BlockSpec(memory_space=pltpu.VMEM)
    part = pl.pallas_call(
        functools.partial(pick_kernel, axes, n),
        out_shape=jax.ShapeDtypeStruct((n, rp + 1, split), f32),
        in_specs=[pl.BlockSpec(memory_space=pltpu.SMEM), pl.BlockSpec(memory_space=pl.ANY)],
        out_specs=vmem,
        scratch_shapes=[pltpu.VMEM((padded, cols), f32), pltpu.SemaphoreType.DMA],
        name="pick",
    )(points, modes)
    chunks = 12 if rows_dev % 96 == 0 else 1
    chunk_shape = pltpu.VMEM((n, rp + 1, split), f32)
    own_shape = pltpu.VMEM((rp + 1, split), f32)
    wide, norms = pl.pallas_call(
        functools.partial(solve_kernel, axes, n),
        out_shape=[
            jax.ShapeDtypeStruct((2 * split, 2 * split), jnp.bfloat16),
            jax.ShapeDtypeStruct((steps, split), f32),
        ],
        in_specs=[vmem, pl.BlockSpec(memory_space=pl.ANY)],
        out_specs=[vmem, vmem],
        scratch_shapes=[
            chunk_shape,
            own_shape,
            chunk_shape,
            chunk_shape,
            chunk_shape,
            own_shape,
            chunk_shape,
            pltpu.VMEM((2 * split, split), f32),
            pltpu.VMEM((chunks, rows_dev // chunks, cols), f32),
            pltpu.VMEM((split, cols), f32),
            pltpu.VMEM((8, split), f32),
        ]
        + [pltpu.SemaphoreType.DMA((n,))] * 4
        + [pltpu.SemaphoreType.DMA((chunks,))],
        compiler_params=pltpu.CompilerParams(collective_id=0, has_side_effects=True),
        name="solve",
    )(part, modes)
    any_space = pl.BlockSpec(memory_space=pl.ANY)
    residual = pl.pallas_call(
        residual_kernel,
        out_shape=jax.ShapeDtypeStruct((rows_dev, split), f32),
        in_specs=[any_space, vmem],
        out_specs=any_space,
        scratch_shapes=[
            pltpu.VMEM((chunks, rows_dev // chunks, cols), f32),
            pltpu.VMEM((chunks, rows_dev // chunks, split), f32),
            pltpu.SemaphoreType.DMA((chunks,)),
            pltpu.SemaphoreType.DMA((chunks,)),
        ],
        name="residual",
    )(modes, wide)
    return residual, norms


def solution(mesh):
    axes = tuple((name, mesh.shape[name]) for name in ("rows", "grp"))
    return jax.shard_map(
        functools.partial(on_device, axes),
        mesh=mesh,
        in_specs=(P(("rows", "grp"), None), P()),
        out_specs=(P(("rows", "grp"), None), P()),
        check_vma=False,
    )
```
